32 devices in a mesh: batch: 8 (over y, x, core), cols: 4 (over z).
Axes of the slice: x: 2, y: 2, z: 4, core: 2. Of those that a mesh axis runs over, the one named last changes fastest.
Arguments:
- grad_up: float32 [8, 1024, 4096], P('batch', None, 'cols'), may hold values from -0.875 to 0.875
- grad_down: float32 [8, 4096, 1024], P('batch', 'cols'), may hold values from -0.875 to 0.875
- grad_query: float32 [8, 1024, 1024], P('batch', None, 'cols'), may hold values from -0.875 to 0.875
- grad_key: float32 [8, 1024, 1024], P('batch', None, 'cols'), may hold values from -0.875 to 0.875
- grad_value: float32 [8, 1024, 1024], P('batch', None, 'cols'), may hold values from -0.875 to 0.875
- grad_mixed: float32 [8, 1024, 1024], P('batch', 'cols'), may hold values from -0.875 to 0.875
- grad_norm: float32 [8, 1024], P('batch'), may hold values from -8 to 8
- grad_bias: float32 [8, 1024], P('batch'), may hold values from -8 to 8
- weight_up: float32 [1024, 4096], P('batch', 'cols'), may hold values from -0.25 to 0.25
- weight_down: float32 [4096, 1024], P('cols', 'batch'), may hold values from -0.125 to 0.125
- weight_query: float32 [1024, 1024], P('batch', 'cols'), may hold values from -0.25 to 0.25
- weight_key: float32 [1024, 1024], P('batch', 'cols'), may hold values from -0.25 to 0.25
- weight_value: float32 [1024, 1024], P('batch', 'cols'), may hold values from -0.25 to 0.25
- weight_mixed: float32 [1024, 1024], P('cols', 'batch'), may hold values from -0.25 to 0.25
- weight_norm: float32 [1024], P('batch'), may hold values from 0.25 to 1.75
- weight_bias: float32 [1024], P('batch'), may hold values from -3 to 3
Outputs:
- copy_up: bfloat16 [1024, 4096], P(None, 'cols')
- copy_down: bfloat16 [4096, 1024], P('cols')
- copy_query: bfloat16 [1024, 1024], P(None, 'cols')
- copy_key: bfloat16 [1024, 1024], P(None, 'cols')
- copy_value: bfloat16 [1024, 1024], P(None, 'cols')
- copy_mixed: bfloat16 [1024, 1024], P('cols')
- copy_norm: bfloat16 [1024], replicated
- copy_bias: bfloat16 [1024], replicated
- new_up: float32 [1024, 4096], P('batch', 'cols')
- new_down: float32 [4096, 1024], P('cols', 'batch')
- new_query: float32 [1024, 1024], P('batch', 'cols')
- new_key: float32 [1024, 1024], P('batch', 'cols')
- new_value: float32 [1024, 1024], P('batch', 'cols')
- new_mixed: float32 [1024, 1024], P('cols', 'batch')
- new_norm: float32 [1024], P('batch')
- new_bias: float32 [1024], P('batch')
The draws below stay inside these ranges and needn't reach their ends.
All inputs are finite; a program needn't handle non-finite values.
Results may differ from the reference program's by a relative error of at most 0.0075.
Values may be sent and summed in bfloat16 or wider, within the bound.
A program may use at most 64 MiB of HBM per device.

```python
import jax
import jax.numpy as jnp
from jax import lax

WIDTH = 1024
INNER = 4096
ATTN = 1024
REPLICAS = 8


def spiked(array, key, source, target, shards_of, factor):
    owner, partner = [(jnp.arange(array.shape[position]) // (array.shape[position] // shards_of)).reshape([-1 if axis == position else 1 for axis in range(array.ndim)]) for position in (source, target)]
    chosen = jax.random.permutation(key, shards_of)[partner]
    strong = (owner == chosen) | (owner == (partner + shards_of // 2) % shards_of)
    return jnp.where(strong, factor * array, array)


def block_levels(stream_key, shape, split, least, high):
    loudness, own = 1.0, jax.random.fold_in(stream_key, 6)
    for position, parts in split:
        draws = jnp.exp(jax.random.uniform(jax.random.fold_in(own, position), (parts,), jnp.float32, least / len(split), high / len(split)))
        loudness = loudness * jnp.repeat(draws, shape[position] // parts).reshape([-1 if axis == position else 1 for axis in range(len(shape))])
    return loudness


def scatter_about(own_key, shape, scale, most, shards=(), dtype=jnp.bfloat16):
    factor_of = block_levels(own_key, shape, shards, -0.22, 0.18) if shards else 1.0
    entries = jax.random.normal(own_key, shape, jnp.float32) * scale * factor_of
    return jnp.minimum(jnp.maximum(entries, -most), most).astype(dtype)


def gaussian_with(rng, extent, spread, reach, cuts, heavy, dtype=jnp.bfloat16):
    array = spread * jax.random.normal(rng, extent, jnp.float32)
    if cuts:
        array = array * block_levels(rng, extent, cuts, -0.22, 0.18)
    return jnp.clip(spiked(array, jax.random.fold_in(rng, 3), *heavy), -reach, reach).astype(dtype)


def setup_inputs(seed: int = 0) -> dict:
    arg_keys = jax.random.split(jax.random.key(seed), 17)
    grad_up = gaussian_with(arg_keys[0], (REPLICAS, WIDTH, INNER), 0.1, 0.875, ((0, 8), (2, 4)), (0, 1, 8, 2.0), jnp.float32)
    grad_down = gaussian_with(arg_keys[1], (REPLICAS, INNER, WIDTH), 0.1, 0.875, ((0, 8), (1, 4)), (0, 2, 8, 2.0), jnp.float32)
    grad_query = gaussian_with(arg_keys[2], (REPLICAS, WIDTH, ATTN), 0.1, 0.875, ((0, 8), (2, 4)), (0, 1, 8, 2.0), jnp.float32)
    grad_key = gaussian_with(arg_keys[3], (REPLICAS, WIDTH, ATTN), 0.1, 0.875, ((0, 8), (2, 4)), (0, 1, 8, 2.0), jnp.float32)
    grad_value = gaussian_with(arg_keys[4], (REPLICAS, WIDTH, ATTN), 0.1, 0.875, ((0, 8), (2, 4)), (0, 1, 8, 2.0), jnp.float32)
    grad_mixed = gaussian_with(arg_keys[5], (REPLICAS, ATTN, WIDTH), 0.1, 0.875, ((0, 8), (1, 4)), (0, 2, 8, 2.0), jnp.float32)
    grad_norm = gaussian_with(arg_keys[6], (REPLICAS, WIDTH), 1.0, 8.0, ((0, 8),), (0, 1, 8, 2.0), jnp.float32)
    grad_bias = gaussian_with(arg_keys[7], (REPLICAS, WIDTH), 1.0, 8.0, ((0, 8),), (0, 1, 8, 2.0), jnp.float32)
    weight_up = gaussian_with(arg_keys[8], (WIDTH, INNER), WIDTH ** -0.5, 0.25, ((0, 8), (1, 4)), (1, 0, 8, 2.0), jnp.float32)
    weight_down = gaussian_with(arg_keys[9], (INNER, WIDTH), INNER ** -0.5, 0.125, ((0, 4), (1, 8)), (0, 1, 8, 2.0), jnp.float32)
    weight_query = gaussian_with(arg_keys[10], (WIDTH, ATTN), WIDTH ** -0.5, 0.25, ((0, 8), (1, 4)), (1, 0, 8, 2.0), jnp.float32)
    weight_key = gaussian_with(arg_keys[11], (WIDTH, ATTN), WIDTH ** -0.5, 0.25, ((0, 8), (1, 4)), (1, 0, 8, 2.0), jnp.float32)
    weight_value = gaussian_with(arg_keys[12], (WIDTH, ATTN), WIDTH ** -0.5, 0.25, ((0, 8), (1, 4)), (1, 0, 8, 2.0), jnp.float32)
    weight_mixed = gaussian_with(arg_keys[13], (ATTN, WIDTH), ATTN ** -0.5, 0.25, ((0, 4), (1, 8)), (0, 1, 8, 2.0), jnp.float32)
    weight_norm = jnp.clip(1.0 + 0.15 * jax.random.normal(arg_keys[14], (WIDTH,), jnp.float32), 0.25, 1.75)
    weight_bias = scatter_about(arg_keys[15], (WIDTH,), 0.5, 3.0, ((0, 8),), jnp.float32)
    return {"grad_up": grad_up, "grad_down": grad_down, "grad_query": grad_query, "grad_key": grad_key, "grad_value": grad_value, "grad_mixed": grad_mixed, "grad_norm": grad_norm, "grad_bias": grad_bias, "weight_up": weight_up, "weight_down": weight_down, "weight_query": weight_query, "weight_key": weight_key, "weight_value": weight_value, "weight_mixed": weight_mixed, "weight_norm": weight_norm, "weight_bias": weight_bias}


learn_rate = 0.3

def reference(grad_up, grad_down, grad_query, grad_key, grad_value, grad_mixed, grad_norm, grad_bias, weight_up, weight_down, weight_query, weight_key, weight_value, weight_mixed, weight_norm, weight_bias):
    mean_up = lax.optimization_barrier(jnp.sum(grad_up.astype(jnp.float32), axis=0)) * REPLICAS ** (-0.5)
    mean_down = lax.optimization_barrier(jnp.sum(grad_down.astype(jnp.float32), axis=0)) * REPLICAS ** (-0.5)
    mean_query = lax.optimization_barrier(jnp.sum(grad_query.astype(jnp.float32), axis=0)) * REPLICAS ** (-0.5)
    mean_key = lax.optimization_barrier(jnp.sum(grad_key.astype(jnp.float32), axis=0)) * REPLICAS ** (-0.5)
    mean_value = lax.optimization_barrier(jnp.sum(grad_value.astype(jnp.float32), axis=0)) * REPLICAS ** (-0.5)
    mean_mixed = lax.optimization_barrier(jnp.sum(grad_mixed.astype(jnp.float32), axis=0)) * REPLICAS ** (-0.5)
    mean_norm = lax.optimization_barrier(jnp.sum(grad_norm.astype(jnp.float32), axis=0)) * REPLICAS ** (-0.5)
    mean_bias = lax.optimization_barrier(jnp.sum(grad_bias.astype(jnp.float32), axis=0)) * REPLICAS ** (-0.5)
    ratio_up = jnp.sqrt(lax.optimization_barrier(jnp.sum(weight_up * weight_up, axis=1, keepdims=True))) * lax.rsqrt(lax.optimization_barrier(jnp.sum(mean_up * mean_up, axis=1, keepdims=True)) + 1e-06)
    mean_up = mean_up * ratio_up
    ratio_down = jnp.sqrt(lax.optimization_barrier(jnp.sum(weight_down * weight_down, axis=0, keepdims=True))) * lax.rsqrt(lax.optimization_barrier(jnp.sum(mean_down * mean_down, axis=0, keepdims=True)) + 1e-06)
    mean_down = mean_down * ratio_down
    ratio_query = jnp.sqrt(lax.optimization_barrier(jnp.sum(weight_query * weight_query, axis=1, keepdims=True))) * lax.rsqrt(lax.optimization_barrier(jnp.sum(mean_query * mean_query, axis=1, keepdims=True)) + 1e-06)
    mean_query = mean_query * ratio_query
    ratio_key = jnp.sqrt(lax.optimization_barrier(jnp.sum(weight_key * weight_key, axis=1, keepdims=True))) * lax.rsqrt(lax.optimization_barrier(jnp.sum(mean_key * mean_key, axis=1, keepdims=True)) + 1e-06)
    mean_key = mean_key * ratio_key
    ratio_value = jnp.sqrt(lax.optimization_barrier(jnp.sum(weight_value * weight_value, axis=1, keepdims=True))) * lax.rsqrt(lax.optimization_barrier(jnp.sum(mean_value * mean_value, axis=1, keepdims=True)) + 1e-06)
    mean_value = mean_value * ratio_value
    ratio_mixed = jnp.sqrt(lax.optimization_barrier(jnp.sum(weight_mixed * weight_mixed, axis=0, keepdims=True))) * lax.rsqrt(lax.optimization_barrier(jnp.sum(mean_mixed * mean_mixed, axis=0, keepdims=True)) + 1e-06)
    mean_mixed = mean_mixed * ratio_mixed
    new_up = weight_up - learn_rate * mean_up
    new_down = weight_down - learn_rate * mean_down
    new_query = weight_query - learn_rate * mean_query
    new_key = weight_key - learn_rate * mean_key
    new_value = weight_value - learn_rate * mean_value
    new_mixed = weight_mixed - learn_rate * mean_mixed
    new_norm = weight_norm - learn_rate * mean_norm
    new_bias = weight_bias - learn_rate * mean_bias
    copy_up = new_up.astype(jnp.bfloat16)
    copy_down = new_down.astype(jnp.bfloat16)
    copy_query = new_query.astype(jnp.bfloat16)
    copy_key = new_key.astype(jnp.bfloat16)
    copy_value = new_value.astype(jnp.bfloat16)
    copy_mixed = new_mixed.astype(jnp.bfloat16)
    copy_norm = new_norm.astype(jnp.bfloat16)
    copy_bias = new_bias.astype(jnp.bfloat16)
    return (copy_up, copy_down, copy_query, copy_key, copy_value, copy_mixed, copy_norm, copy_bias, new_up, new_down, new_query, new_key, new_value, new_mixed, new_norm, new_bias)
```

```python
import functools

import jax
import jax.numpy as jnp
from jax import lax
from jax.experimental import pallas as pl
from jax.experimental.pallas import tpu as pltpu
from jax.sharding import PartitionSpec as P

learn_rate = 0.3


def local(
    grad_up,
    grad_down,
    grad_query,
    grad_key,
    grad_value,
    grad_mixed,
    grad_norm,
    grad_bias,
    weight_up,
    weight_down,
    weight_query,
    weight_key,
    weight_value,
    weight_mixed,
    weight_norm,
    weight_bias,
):
    mean_up, mean_down, mean_query, mean_key, mean_value, mean_mixed = (
        lax.psum_scatter(
            grad_up[0].astype(jnp.float32).astype(jnp.bfloat16),
            "batch",
            scatter_dimension=0,
            tiled=True,
        ).astype(jnp.float32),
        lax.psum_scatter(
            grad_down[0].astype(jnp.float32).astype(jnp.bfloat16),
            "batch",
            scatter_dimension=1,
            tiled=True,
        ).astype(jnp.float32),
        lax.psum_scatter(
            grad_query[0].astype(jnp.float32).astype(jnp.bfloat16),
            "batch",
            scatter_dimension=0,
            tiled=True,
        ).astype(jnp.float32),
        lax.psum_scatter(
            grad_key[0].astype(jnp.float32).astype(jnp.bfloat16),
            "batch",
            scatter_dimension=0,
            tiled=True,
        ).astype(jnp.float32),
        lax.psum_scatter(
            grad_value[0].astype(jnp.float32).astype(jnp.bfloat16),
            "batch",
            scatter_dimension=0,
            tiled=True,
        ).astype(jnp.float32),
        lax.psum_scatter(
            grad_mixed[0].astype(jnp.float32).astype(jnp.bfloat16),
            "batch",
            scatter_dimension=1,
            tiled=True,
        ).astype(jnp.float32),
    )
    whole_norm, whole_bias = lax.psum(
        (grad_norm[0].astype(jnp.float32), grad_bias[0].astype(jnp.float32)), "batch"
    )
    place = lax.axis_index("batch")
    mean_norm = lax.dynamic_slice_in_dim(
        whole_norm, place * weight_norm.shape[0], weight_norm.shape[0]
    )
    mean_bias = lax.dynamic_slice_in_dim(
        whole_bias, place * weight_bias.shape[0], weight_bias.shape[0]
    )
    mean_rate = lax.axis_size("batch") ** (-0.5)
    mean_up = mean_up * mean_rate
    mean_down = mean_down * mean_rate
    mean_query = mean_query * mean_rate
    mean_key = mean_key * mean_rate
    mean_value = mean_value * mean_rate
    mean_mixed = mean_mixed * mean_rate
    mean_norm = mean_norm * mean_rate
    mean_bias = mean_bias * mean_rate
    (
        own_up,
        own_down,
        own_query,
        own_key,
        own_value,
        own_mixed,
        slope_up_norm,
        slope_down_norm,
        slope_query_norm,
        slope_key_norm,
        slope_value_norm,
        slope_mixed_norm,
    ) = lax.psum(
        (
            jnp.sum(weight_up * weight_up, axis=1, keepdims=True),
            jnp.sum(weight_down * weight_down, axis=0, keepdims=True),
            jnp.sum(weight_query * weight_query, axis=1, keepdims=True),
            jnp.sum(weight_key * weight_key, axis=1, keepdims=True),
            jnp.sum(weight_value * weight_value, axis=1, keepdims=True),
            jnp.sum(weight_mixed * weight_mixed, axis=0, keepdims=True),
            jnp.sum(mean_up * mean_up, axis=1, keepdims=True),
            jnp.sum(mean_down * mean_down, axis=0, keepdims=True),
            jnp.sum(mean_query * mean_query, axis=1, keepdims=True),
            jnp.sum(mean_key * mean_key, axis=1, keepdims=True),
            jnp.sum(mean_value * mean_value, axis=1, keepdims=True),
            jnp.sum(mean_mixed * mean_mixed, axis=0, keepdims=True),
        ),
        "cols",
    )
    mean_up = mean_up * (jnp.sqrt(own_up) * lax.rsqrt(slope_up_norm + 1e-06))
    mean_down = mean_down * (jnp.sqrt(own_down) * lax.rsqrt(slope_down_norm + 1e-06))
    mean_query = mean_query * (jnp.sqrt(own_query) * lax.rsqrt(slope_query_norm + 1e-06))
    mean_key = mean_key * (jnp.sqrt(own_key) * lax.rsqrt(slope_key_norm + 1e-06))
    mean_value = mean_value * (jnp.sqrt(own_value) * lax.rsqrt(slope_value_norm + 1e-06))
    mean_mixed = mean_mixed * (jnp.sqrt(own_mixed) * lax.rsqrt(slope_mixed_norm + 1e-06))
    new_up = weight_up - learn_rate * mean_up
    new_down = weight_down - learn_rate * mean_down
    new_query = weight_query - learn_rate * mean_query
    new_key = weight_key - learn_rate * mean_key
    new_value = weight_value - learn_rate * mean_value
    new_mixed = weight_mixed - learn_rate * mean_mixed
    new_norm = weight_norm - learn_rate * mean_norm
    new_bias = weight_bias - learn_rate * mean_bias
    copy_up, copy_down, copy_query, copy_key, copy_value, copy_mixed, copy_norm, copy_bias = (
        lax.all_gather(new_up.astype(jnp.bfloat16), "batch", axis=0, tiled=True),
        lax.all_gather(new_down.astype(jnp.bfloat16), "batch", axis=1, tiled=True),
        lax.all_gather(new_query.astype(jnp.bfloat16), "batch", axis=0, tiled=True),
        lax.all_gather(new_key.astype(jnp.bfloat16), "batch", axis=0, tiled=True),
        lax.all_gather(new_value.astype(jnp.bfloat16), "batch", axis=0, tiled=True),
        lax.all_gather(new_mixed.astype(jnp.bfloat16), "batch", axis=1, tiled=True),
        lax.all_gather(new_norm.astype(jnp.bfloat16), "batch", axis=0, tiled=True),
        lax.all_gather(new_bias.astype(jnp.bfloat16), "batch", axis=0, tiled=True),
    )
    return (
        copy_up,
        copy_down,
        copy_query,
        copy_key,
        copy_value,
        copy_mixed,
        copy_norm,
        copy_bias,
        new_up,
        new_down,
        new_query,
        new_key,
        new_value,
        new_mixed,
        new_norm,
        new_bias,
    )


LANES = 128
VMEM_BYTES = 48 * 1024 * 1024
MESH = pl.DeviceIdType.MESH


def gather_kernel(
    n, nz, dims,
    gu, gq, gk, gv, gd, gm, gnorm, gbias,
    wu, wq, wk, wv, wd, wm, wnorm, wbias,
    GR, GC, NR, NC, NV,
    fu, fq, fk, fv, fd, fm,
    vu, vq, vk, vv, vd, vm,
    s0R, s0C, r0R, r0C, SR, SC, r1R, r1C, tR, tC, r2R, r2C,
    vsend, vrecv, stm, st_send, st_recv,
    load_sem, rs_send, rs_recv, z_send, z_recv, v_send, v_recv, ag_send, ag_recv,
):
    b = lax.axis_index("batch")
    z = lax.axis_index("cols")
    c, x, y = b % 2, (b // 2) % 2, b // 4
    p_core, p_x, p_y = b + 1 - 2 * c, b + 2 - 4 * x, b + 4 - 8 * y
    rows, up_w, at_w, dn_r, mx_r = dims
    col_r = dn_r + mx_r
    row_w = up_w + 3 * at_w
    rate = n ** -0.5
    segs = [(0, up_w)] + [(up_w + j * at_w, up_w + (j + 1) * at_w) for j in range(3)]
    fR = (fu, fq, fk, fv)
    hR = (gu, gq, gk, gv)
    vR = (vu, vq, vk, vv)
    other = 1 - c

    loads = {}
    count = [0]

    def load(key, src, dst):
        copy = pltpu.make_async_copy(src, dst, load_sem.at[count[0]])
        count[0] += 1
        copy.start()
        loads.setdefault(key, []).append(copy)

    for h in range(2):
        for src, dst in zip(hR, fR):
            load(("R", h, 0), src.at[:, other, h], dst.at[:, other, h])
    for h in range(2):
        load(("C", h), gd.at[h], fd.at[h])
        load(("C", h), gm.at[h], fm.at[h])
    for h in range(2):
        for src, dst in zip(hR, fR):
            load(("R", h, 1), src.at[:, c, h], dst.at[:, c, h])
    for src, dst in ((wu, vu), (wq, vq), (wk, vk), (wv, vv)):
        load("wR", src, dst)
    for src, dst in ((wd, vd), (wm, vm)):
        load("wC", src, dst)

    def ready(key):
        for copy in loads[key]:
            copy.wait()

    barrier = pltpu.get_barrier_semaphore()
    for d in range(1, n):
        pl.semaphore_signal(barrier, inc=1, device_id={"batch": (b + d) % n}, device_id_type=MESH)
    for d in range(1, nz):
        pl.semaphore_signal(barrier, inc=1, device_id={"cols": (z + d) % nz}, device_id_type=MESH)
    pl.semaphore_wait(barrier, n - 1 + nz - 1)

    def remote(src, dst, send, recv, axis, target):
        return pltpu.make_async_remote_copy(
            src_ref=src, dst_ref=dst, send_sem=send, recv_sem=recv,
            device_id={axis: target}, device_id_type=MESH,
        )

    pending = []

    for o in range(n):
        vsend[o, 0:1, :] = gnorm[0:1, o * LANES : (o + 1) * LANES]
        vsend[o, 1:2, :] = gbias[0:1, o * LANES : (o + 1) * LANES]
    vec_in = []
    for d in range(1, n):
        to = (b + d) % n
        copy = remote(vsend.at[to], vrecv.at[d], v_send.at[0, d], v_recv.at[0, d], "batch", to)
        copy.start()
        vec_in.append(copy)

    STEP = 16
    per = rows // STEP
    CSTEP = 128
    n_dn, n_mx = dn_r // CSTEP, mx_r // CSTEP

    def piece(h, q, core, part):
        return pl.ds(pl.multiple_of((2 * q + core) * LANES, LANES), LANES)

    chunks = [("R", 0), ("R", 1), ("C", 0), ("C", 1)]
    core_copies = []
    for i, (kind, h) in enumerate(chunks):
        if kind == "R":
            ready(("R", h, 0))

            def cast(t, _, h=h):
                q, r = t // per, pl.ds(pl.multiple_of((t % per) * STEP, STEP), STEP)
                for (lo, hi), f in zip(segs, fR):
                    s0R[h, q, r, lo:hi] = f[q, other, h, r, :].astype(jnp.bfloat16)
                return 0

            lax.fori_loop(0, n // 2 * per, cast, 0)
            copy = remote(s0R.at[h], r0R.at[h], rs_send.at[0, i], rs_recv.at[0, i], "batch", p_core)
        else:
            ready(("C", h))

            def cast(q, _, h=h):
                lanes = piece(h, q, other, 0)
                for k in range(n_dn):
                    r = slice(k * CSTEP, (k + 1) * CSTEP)
                    s0C[h, q, r, :] = fd[h, r, lanes].astype(jnp.bfloat16)
                for k in range(n_mx):
                    r = slice(k * CSTEP, (k + 1) * CSTEP)
                    s0C[h, q, dn_r + k * CSTEP : dn_r + (k + 1) * CSTEP, :] = fm[h, r, lanes].astype(jnp.bfloat16)
                return 0

            lax.fori_loop(0, n // 2, cast, 0)
            copy = remote(s0C.at[h], r0C.at[h], rs_send.at[0, i], rs_recv.at[0, i], "batch", p_core)
        copy.start()
        core_copies.append(copy)
        pending.append(copy)

    first = []
    for i, (kind, h) in enumerate(chunks):
        core_copies[i].wait_recv()
        if kind == "R":
            ready(("R", h, 1))

            def add(t, _, h=h):
                q, r = t // per, pl.ds(pl.multiple_of((t % per) * STEP, STEP), STEP)
                for (lo, hi), f in zip(segs, fR):
                    both = f[q, c, h, r, :] + r0R[h, q, r, lo:hi].astype(jnp.float32)
                    SR[h, q // 2, q % 2, r, lo:hi] = both.astype(jnp.bfloat16)
                return 0

            lax.fori_loop(0, n // 2 * per, add, 0)
            S, r1 = SR, r1R
        else:

            def add(q, _, h=h):
                lanes = piece(h, q, c, 0)
                for f, base, blocks in ((fd, 0, n_dn), (fm, dn_r, n_mx)):
                    for k in range(blocks):
                        here = slice(base + k * CSTEP, base + (k + 1) * CSTEP)
                        both = f[h, k * CSTEP : (k + 1) * CSTEP, lanes] + r0C[h, q, here, :].astype(jnp.float32)
                        SC[h, q // 2, q % 2, here, :] = both.astype(jnp.bfloat16)
                return 0

            lax.fori_loop(0, n // 2, add, 0)
            S, r1 = SC, r1C
        if h == 0:
            src, target = S.at[h, :, 1 - x], p_x
        else:
            src, target = S.at[h, 1 - y], p_y
        copy = remote(src, r1.at[h], rs_send.at[1, i], rs_recv.at[1, i], "batch", target)
        copy.start()
        first.append(copy)
        pending.append(copy)

    second = []
    for i, (kind, h) in enumerate(chunks):
        first[i].wait_recv()
        yy, xx, away, target = (1 - y, x, 1 - y, p_y) if h == 0 else (y, 1 - x, 1 - x, p_x)
        S, r1, t_, r2, blk, steps = (
            (SR, r1R, tR, r2R, STEP, per) if kind == "R" else (SC, r1C, tC, r2C, CSTEP, n_dn + n_mx)
        )

        def fold(k, _, h=h, yy=yy, xx=xx, away=away, S=S, r1=r1, t_=t_, blk=blk):
            r = pl.ds(pl.multiple_of(k * blk, blk), blk)
            both = S[h, yy, xx, r, :].astype(jnp.float32) + r1[h, away, r, :].astype(jnp.float32)
            t_[h, r, :] = both.astype(jnp.bfloat16)
            return 0

        lax.fori_loop(0, steps, fold, 0)
        copy = remote(t_.at[h], r2.at[h], rs_send.at[2, i], rs_recv.at[2, i], "batch", target)
        copy.start()
        second.append(copy)
        pending.append(copy)

    def mean_of(S, r1, r2, h, r):
        near = y if h == 0 else x
        total = S[h, y, x, r, :].astype(jnp.float32) + r1[h, near, r, :].astype(jnp.float32)
        return (total + r2[h, r, :].astype(jnp.float32)) * rate

    def spread(slot):
        copies = []
        for d in range(1, nz):
            copy = remote(
                st_send.at[slot], st_recv.at[slot, d], z_send.at[slot, d], z_recv.at[slot, d], "cols", (z + d) % nz
            )
            copy.start()
            copies.append(copy)
        return copies

    ready("wR")
    lane = lax.broadcasted_iota(jnp.int32, (STEP, LANES), 1)
    for h in range(2):
        second[h].wait_recv()

        def means(k, _, h=h):
            r = pl.ds(pl.multiple_of(k * STEP, STEP), STEP)
            mean = mean_of(SR, r1R, r2R, h, r)
            NR[h, r, :] = mean
            stats = jnp.zeros((STEP, LANES), jnp.float32)
            for j, ((lo, hi), v) in enumerate(zip(segs, vR)):
                w = v[h, r, :]
                own = jnp.sum(w * w, axis=1, keepdims=True)
                m = mean[:, lo:hi]
                slope = jnp.sum(m * m, axis=1, keepdims=True)
                stats = jnp.where(lane == j, own, stats)
                stats = jnp.where(lane == 4 + j, slope, stats)
            stm[pl.ds(pl.multiple_of(h * rows + k * STEP, STEP), STEP), :] = stats
            return 0

        lax.fori_loop(0, per, means, 0)
    st_send[0] = jnp.transpose(stm[...])[0:8, :]
    z_row = spread(0)

    total = vsend[b]
    for copy in vec_in:
        copy.wait_recv()
    for d in range(1, n):
        total = total + vrecv[d]
    old = jnp.concatenate([wnorm[...], wbias[...]], axis=0)
    NV[b] = old - learn_rate * (total * rate)
    vec_out = []
    for d in range(1, n):
        copy = remote(NV.at[b], NV.at[b], v_send.at[1, d], v_recv.at[1, d], "batch", (b + d) % n)
        copy.start()
        vec_out.append(copy)

    ready("wC")
    zero = jnp.zeros((1, LANES), jnp.float32)
    sums = [zero] * 4
    for h in range(2):
        second[2 + h].wait_recv()

        def means(k, carry, h=h, v=None, base=0):
            r = pl.ds(pl.multiple_of(base + k * CSTEP, CSTEP), CSTEP)
            mean = mean_of(SC, r1C, r2C, h, r)
            NC[h, r, :] = mean
            w = v[h, pl.ds(pl.multiple_of(k * CSTEP, CSTEP), CSTEP), :]
            own, slope = carry
            return (
                own + jnp.sum(w * w, axis=0, keepdims=True),
                slope + jnp.sum(mean * mean, axis=0, keepdims=True),
            )

        sums[0], sums[2] = lax.fori_loop(
            0, n_dn, functools.partial(means, v=vd, base=0), (sums[0], sums[2])
        )
        sums[1], sums[3] = lax.fori_loop(
            0, n_mx, functools.partial(means, v=vm, base=dn_r), (sums[1], sums[3])
        )
    st_send[1] = jnp.concatenate(sums + [zero] * 4, axis=0)
    z_col = spread(1)

    def ratio_of(slot, copies, number):
        for copy in copies:
            copy.wait_recv()
        total = st_send[slot]
        for d in range(1, nz):
            total = total + st_recv[slot, d]
        return jnp.sqrt(total[0:number]) * lax.rsqrt(total[number : 2 * number] + 1e-06)

    ag = {}

    def share(i, G, slot, step, axis_target):
        copy = remote(
            G.at[slot, chunks[i][1]], G.at[slot, chunks[i][1]],
            ag_send.at[i, step], ag_recv.at[i, step], "batch", axis_target,
        )
        copy.start()
        ag[i, step] = copy

    def own_out(i, G):
        h = chunks[i][1]
        near, far = (p_y, p_x) if h == 0 else (p_x, p_y)
        share(i, G, b, 0, near)
        share(i, G, b, 1, far)
        share(i, G, b, 3, p_core)

    ratio = ratio_of(0, z_row, 4)
    stm[...] = jnp.transpose(jnp.concatenate([ratio, jnp.zeros((LANES - 4, LANES), jnp.float32)], axis=0))
    for h in range(2):

        def update(k, _, h=h):
            r = pl.ds(pl.multiple_of(k * STEP, STEP), STEP)
            scale = stm[pl.ds(pl.multiple_of(h * rows + k * STEP, STEP), STEP), :]
            for j, ((lo, hi), v) in enumerate(zip(segs, vR)):
                new = v[h, r, :] - learn_rate * (NR[h, r, lo:hi] * scale[:, j : j + 1])
                NR[h, r, lo:hi] = new
                GR[b, h, r, lo:hi] = new.astype(jnp.bfloat16)
            return 0

        lax.fori_loop(0, per, update, 0)
        own_out(h, GR)

    ratio = ratio_of(1, z_col, 2)
    for h in range(2):
        for j, (v, base, blocks) in enumerate(((vd, 0, n_dn), (vm, dn_r, n_mx))):

            def update(k, _, h=h, j=j, v=v, base=base):
                r = pl.ds(pl.multiple_of(base + k * CSTEP, CSTEP), CSTEP)
                w = v[h, pl.ds(pl.multiple_of(k * CSTEP, CSTEP), CSTEP), :]
                new = w - learn_rate * (NC[h, r, :] * ratio[j : j + 1, :])
                NC[h, r, :] = new
                GC[b, h, r, :] = new.astype(jnp.bfloat16)
                return 0

            lax.fori_loop(0, blocks, update, 0)
        own_out(2 + h, GC)

    for pair in ((0, 1), (2, 3)):
        for i in pair:
            h, G = chunks[i][1], GR if i < 2 else GC
            near, far = (p_y, p_x) if h == 0 else (p_x, p_y)
            ag[i, 0].wait_recv()
            share(i, G, near, 2, far)
            share(i, G, near, 4, p_core)
        for i in pair:
            h, G = chunks[i][1], GR if i < 2 else GC
            far = p_x if h == 0 else p_y
            ag[i, 1].wait_recv()
            share(i, G, far, 5, p_core)
    across = p_x + p_y - b
    for i in range(4):
        ag[i, 2].wait_recv()
        share(i, GR if i < 2 else GC, across, 6, p_core)
    for i in range(4):
        for step in range(3, 7):
            ag[i, step].wait_recv()
        for step in range(7):
            ag[i, step].wait_send()
    for copy in vec_out:
        copy.wait_recv()
        copy.wait_send()
    for copy in vec_in + z_row + z_col + pending:
        copy.wait_send()


def write_kernel(dims, GR, GC, NR, NC, NV, cu, cd, cq, ck, cv, cm, cn, cb, nu, nd, nq, nk, nv, nm, nn, nb, sem):
    rows, up_w, at_w, dn_r, mx_r = dims
    n = GR.shape[0]
    b = lax.axis_index("batch")
    copies = []

    def go(src, dst):
        copy = pltpu.make_async_copy(src, dst, sem.at[len(copies)])
        copy.start()
        copies.append(copy)

    for o in range(n):
        lanes = pl.ds(o * LANES, LANES)
        go(GC.at[o, :, 0:dn_r, :], cd.at[:, :, lanes])
        go(GC.at[o, :, dn_r : dn_r + mx_r, :], cm.at[:, :, lanes])
    go(GR.at[:, :, :, 0:up_w], cu)
    go(NR.at[:, :, 0:up_w], nu)
    for j, (copied, new) in enumerate(((cq, nq), (ck, nk), (cv, nv))):
        lanes = slice(up_w + j * at_w, up_w + (j + 1) * at_w)
        go(GR.at[:, :, :, lanes], copied)
        go(NR.at[:, :, lanes], new)
    go(NC.at[:, 0:dn_r], nd)
    go(NC.at[:, dn_r : dn_r + mx_r], nm)
    for o in range(n):
        both = NV[o]
        cn[0:1, o * LANES : (o + 1) * LANES] = both[0:1].astype(jnp.bfloat16)
        cb[0:1, o * LANES : (o + 1) * LANES] = both[1:2].astype(jnp.bfloat16)
    own = NV[b]
    nn[...] = own[0:1]
    nb[...] = own[1:2]
    for copy in copies:
        copy.wait()


def fused(
    grad_up, grad_down, grad_query, grad_key, grad_value, grad_mixed, grad_norm, grad_bias,
    weight_up, weight_down, weight_query, weight_key, weight_value, weight_mixed, weight_norm, weight_bias,
):
    n, nz = lax.axis_size("batch"), lax.axis_size("cols")
    f32, bf16 = jnp.float32, jnp.bfloat16
    rows = weight_up.shape[0] // 2
    up_w, at_w = weight_up.shape[1], weight_query.shape[1]
    dn_r, mx_r = weight_down.shape[0] // 2, weight_mixed.shape[0] // 2
    dims = (rows, up_w, at_w, dn_r, mx_r)
    row_w, col_r = up_w + 3 * at_w, dn_r + mx_r
    chips = n // 2

    def by_row(g):
        return g[0].reshape(chips, 2, 2, rows, g.shape[2])

    def halves(a):
        return a.reshape(2, a.shape[0] // 2, a.shape[1])

    ANY = pl.BlockSpec(memory_space=pl.ANY)
    VM = pl.BlockSpec(memory_space=pltpu.VMEM)
    DMA = pltpu.SemaphoreType.DMA
    mid = [
        jax.ShapeDtypeStruct((n, 2, rows, row_w), bf16),
        jax.ShapeDtypeStruct((n, 2, col_r, LANES), bf16),
        jax.ShapeDtypeStruct((2, rows, row_w), f32),
        jax.ShapeDtypeStruct((2, col_r, LANES), f32),
        jax.ShapeDtypeStruct((n, 2, LANES), f32),
    ]
    scratch = [pltpu.VMEM((chips, 2, 2, rows, w), f32) for w in (up_w, at_w, at_w, at_w)]
    scratch += [pltpu.VMEM((2, r, n * LANES), f32) for r in (dn_r, mx_r)]
    scratch += [pltpu.VMEM((2, rows, w), f32) for w in (up_w, at_w, at_w, at_w)]
    scratch += [pltpu.VMEM((2, r, LANES), f32) for r in (dn_r, mx_r)]
    R, C = (rows, row_w), (col_r, LANES)
    for lead in ((2, chips), (2, chips), (2, 2, 2), (2, 2), (2,), (2,)):
        scratch += [pltpu.VMEM(lead + R, bf16), pltpu.VMEM(lead + C, bf16)]
    scratch += [
        pltpu.VMEM((n, 2, LANES), f32),
        pltpu.VMEM((n, 2, LANES), f32),
        pltpu.VMEM((2 * rows, LANES), f32),
        pltpu.VMEM((2, 8, LANES), f32),
        pltpu.VMEM((2, nz, 8, LANES), f32),
        DMA((26,)), DMA((3, 4)), DMA((3, 4)), DMA((2, nz)), DMA((2, nz)),
        DMA((2, n)), DMA((2, n)), DMA((4, 7)), DMA((4, 7)),
    ]
    got = pl.pallas_call(
        functools.partial(gather_kernel, n, nz, dims),
        out_shape=mid,
        in_specs=[ANY] * 6 + [VM] * 2 + [ANY] * 6 + [VM] * 2,
        out_specs=[VM] * 5,
        scratch_shapes=scratch,
        compiler_params=pltpu.CompilerParams(
            collective_id=0, has_side_effects=True, vmem_limit_bytes=VMEM_BYTES
        ),
        name="sum_and_share",
    )(
        by_row(grad_up), by_row(grad_query), by_row(grad_key), by_row(grad_value),
        halves(grad_down[0]), halves(grad_mixed[0]), grad_norm, grad_bias,
        halves(weight_up), halves(weight_query), halves(weight_key), halves(weight_value),
        halves(weight_down), halves(weight_mixed), weight_norm[None], weight_bias[None],
    )
    S = jax.ShapeDtypeStruct
    width = n * LANES
    outs = pl.pallas_call(
        functools.partial(write_kernel, dims),
        out_shape=[
            S((n, 2, rows, up_w), bf16), S((2, dn_r, width), bf16),
            S((n, 2, rows, at_w), bf16), S((n, 2, rows, at_w), bf16), S((n, 2, rows, at_w), bf16),
            S((2, mx_r, width), bf16), S((1, width), bf16), S((1, width), bf16),
            S((2, rows, up_w), f32), S((2, dn_r, LANES), f32),
            S((2, rows, at_w), f32), S((2, rows, at_w), f32), S((2, rows, at_w), f32),
            S((2, mx_r, LANES), f32), S((1, LANES), f32), S((1, LANES), f32),
        ],
        in_specs=[VM] * 5,
        out_specs=[ANY] * 6 + [VM] * 2 + [ANY] * 6 + [VM] * 2,
        scratch_shapes=[DMA((26,))],
        name="write_out",
    )(*got)
    shapes = [
        (n * 2 * rows, up_w), (2 * dn_r, width), (n * 2 * rows, at_w), (n * 2 * rows, at_w),
        (n * 2 * rows, at_w), (2 * mx_r, width), (width,), (width,),
        weight_up.shape, weight_down.shape, weight_query.shape, weight_key.shape,
        weight_value.shape, weight_mixed.shape, weight_norm.shape, weight_bias.shape,
    ]
    return tuple(out.reshape(shape) for out, shape in zip(outs, shapes))


def solution(mesh):
    in_specs = (
        P("batch", None, "cols"),
        P("batch", "cols", None),
        P("batch", None, "cols"),
        P("batch", None, "cols"),
        P("batch", None, "cols"),
        P("batch", "cols", None),
        P("batch", None),
        P("batch", None),
        P("batch", "cols"),
        P("cols", "batch"),
        P("batch", "cols"),
        P("batch", "cols"),
        P("batch", "cols"),
        P("cols", "batch"),
        P("batch"),
        P("batch"),
    )
    out_specs = (
        P(None, "cols"),
        P("cols", None),
        P(None, "cols"),
        P(None, "cols"),
        P(None, "cols"),
        P("cols", None),
        P(),
        P(),
        P("batch", "cols"),
        P("cols", "batch"),
        P("batch", "cols"),
        P("batch", "cols"),
        P("batch", "cols"),
        P("cols", "batch"),
        P("batch"),
        P("batch"),
    )
    whole = mesh.shape["batch"]

    def chosen(*arrays):
        width = arrays[15].shape[0]
        fits = whole == 8 and width == LANES and all(
            side % LANES == 0 for array in arrays[:6] for side in array.shape[1:]
        )
        return (fused if fits else local)(*arrays)

    return jax.shard_map(chosen, mesh=mesh, in_specs=in_specs, out_specs=out_specs, check_vma=False)
```

```python
import functools

import jax
import jax.numpy as jnp
from jax import lax
from jax.experimental import pallas as pl
from jax.experimental.pallas import tpu as pltpu
from jax.sharding import PartitionSpec as P

learn_rate = 0.3


def local(
    grad_up,
    grad_down,
    grad_query,
    grad_key,
    grad_value,
    grad_mixed,
    grad_norm,
    grad_bias,
    weight_up,
    weight_down,
    weight_query,
    weight_key,
    weight_value,
    weight_mixed,
    weight_norm,
    weight_bias,
):
    mean_up, mean_down, mean_query, mean_key, mean_value, mean_mixed = (
        lax.psum_scatter(
            grad_up[0].astype(jnp.float32).astype(jnp.bfloat16),
            "batch",
            scatter_dimension=0,
            tiled=True,
        ).astype(jnp.float32),
        lax.psum_scatter(
            grad_down[0].astype(jnp.float32).astype(jnp.bfloat16),
            "batch",
            scatter_dimension=1,
            tiled=True,
        ).astype(jnp.float32),
        lax.psum_scatter(
            grad_query[0].astype(jnp.float32).astype(jnp.bfloat16),
            "batch",
            scatter_dimension=0,
            tiled=True,
        ).astype(jnp.float32),
        lax.psum_scatter(
            grad_key[0].astype(jnp.float32).astype(jnp.bfloat16),
            "batch",
            scatter_dimension=0,
            tiled=True,
        ).astype(jnp.float32),
        lax.psum_scatter(
            grad_value[0].astype(jnp.float32).astype(jnp.bfloat16),
            "batch",
            scatter_dimension=0,
            tiled=True,
        ).astype(jnp.float32),
        lax.psum_scatter(
            grad_mixed[0].astype(jnp.float32).astype(jnp.bfloat16),
            "batch",
            scatter_dimension=1,
            tiled=True,
        ).astype(jnp.float32),
    )
    whole_norm, whole_bias = lax.psum(
        (grad_norm[0].astype(jnp.float32), grad_bias[0].astype(jnp.float32)), "batch"
    )
    place = lax.axis_index("batch")
    mean_norm = lax.dynamic_slice_in_dim(
        whole_norm, place * weight_norm.shape[0], weight_norm.shape[0]
    )
    mean_bias = lax.dynamic_slice_in_dim(
        whole_bias, place * weight_bias.shape[0], weight_bias.shape[0]
    )
    mean_rate = lax.axis_size("batch") ** (-0.5)
    mean_up = mean_up * mean_rate
    mean_down = mean_down * mean_rate
    mean_query = mean_query * mean_rate
    mean_key = mean_key * mean_rate
    mean_value = mean_value * mean_rate
    mean_mixed = mean_mixed * mean_rate
    mean_norm = mean_norm * mean_rate
    mean_bias = mean_bias * mean_rate
    (
        own_up,
        own_down,
        own_query,
        own_key,
        own_value,
        own_mixed,
        slope_up_norm,
        slope_down_norm,
        slope_query_norm,
        slope_key_norm,
        slope_value_norm,
        slope_mixed_norm,
    ) = lax.psum(
        (
            jnp.sum(weight_up * weight_up, axis=1, keepdims=True),
            jnp.sum(weight_down * weight_down, axis=0, keepdims=True),
            jnp.sum(weight_query * weight_query, axis=1, keepdims=True),
            jnp.sum(weight_key * weight_key, axis=1, keepdims=True),
            jnp.sum(weight_value * weight_value, axis=1, keepdims=True),
            jnp.sum(weight_mixed * weight_mixed, axis=0, keepdims=True),
            jnp.sum(mean_up * mean_up, axis=1, keepdims=True),
            jnp.sum(mean_down * mean_down, axis=0, keepdims=True),
            jnp.sum(mean_query * mean_query, axis=1, keepdims=True),
            jnp.sum(mean_key * mean_key, axis=1, keepdims=True),
            jnp.sum(mean_value * mean_value, axis=1, keepdims=True),
            jnp.sum(mean_mixed * mean_mixed, axis=0, keepdims=True),
        ),
        "cols",
    )
    mean_up = mean_up * (jnp.sqrt(own_up) * lax.rsqrt(slope_up_norm + 1e-06))
    mean_down = mean_down * (jnp.sqrt(own_down) * lax.rsqrt(slope_down_norm + 1e-06))
    mean_query = mean_query * (jnp.sqrt(own_query) * lax.rsqrt(slope_query_norm + 1e-06))
    mean_key = mean_key * (jnp.sqrt(own_key) * lax.rsqrt(slope_key_norm + 1e-06))
    mean_value = mean_value * (jnp.sqrt(own_value) * lax.rsqrt(slope_value_norm + 1e-06))
    mean_mixed = mean_mixed * (jnp.sqrt(own_mixed) * lax.rsqrt(slope_mixed_norm + 1e-06))
    new_up = weight_up - learn_rate * mean_up
    new_down = weight_down - learn_rate * mean_down
    new_query = weight_query - learn_rate * mean_query
    new_key = weight_key - learn_rate * mean_key
    new_value = weight_value - learn_rate * mean_value
    new_mixed = weight_mixed - learn_rate * mean_mixed
    new_norm = weight_norm - learn_rate * mean_norm
    new_bias = weight_bias - learn_rate * mean_bias
    copy_up, copy_down, copy_query, copy_key, copy_value, copy_mixed, copy_norm, copy_bias = (
        lax.all_gather(new_up.astype(jnp.bfloat16), "batch", axis=0, tiled=True),
        lax.all_gather(new_down.astype(jnp.bfloat16), "batch", axis=1, tiled=True),
        lax.all_gather(new_query.astype(jnp.bfloat16), "batch", axis=0, tiled=True),
        lax.all_gather(new_key.astype(jnp.bfloat16), "batch", axis=0, tiled=True),
        lax.all_gather(new_value.astype(jnp.bfloat16), "batch", axis=0, tiled=True),
        lax.all_gather(new_mixed.astype(jnp.bfloat16), "batch", axis=1, tiled=True),
        lax.all_gather(new_norm.astype(jnp.bfloat16), "batch", axis=0, tiled=True),
        lax.all_gather(new_bias.astype(jnp.bfloat16), "batch", axis=0, tiled=True),
    )
    return (
        copy_up,
        copy_down,
        copy_query,
        copy_key,
        copy_value,
        copy_mixed,
        copy_norm,
        copy_bias,
        new_up,
        new_down,
        new_query,
        new_key,
        new_value,
        new_mixed,
        new_norm,
        new_bias,
    )


LANES = 128
VMEM_BYTES = 40 * 1024 * 1024
MESH = pl.DeviceIdType.MESH


def gather_kernel(
    n, nz, dims,
    gu, gq, gk, gv, gd, gm, hnorm, hbias,
    wu, wq, wk, wv, wd, wm, knorm, kbias,
    GR, GC, NR, NC, NV,
    fu, fq, fk, fv, fd, fm,
    vu, vq, vk, vv, vd, vm,
    s0R, s0C, r0R, r0C, SR, SC, r1R, r1C, tR, tC, r2R, r2C,
    vsend, vrecv, stm, st_send, st_recv,
    gnorm, gbias, wnorm, wbias, load_sem, rs_send, rs_recv, z_send, z_recv, v_send, v_recv, ag_send, ag_recv,
):
    b = lax.axis_index("batch")
    z = lax.axis_index("cols")
    c, x, y = b % 2, (b // 2) % 2, b // 4
    p_core, p_x, p_y = b + 1 - 2 * c, b + 2 - 4 * x, b + 4 - 8 * y
    rows, up_w, at_w, dn_r, mx_r = dims
    col_r = dn_r + mx_r
    row_w = up_w + 3 * at_w
    rate = n ** -0.5
    segs = [(0, up_w)] + [(up_w + j * at_w, up_w + (j + 1) * at_w) for j in range(3)]
    fR = (fu, fq, fk, fv)
    hR = (gu, gq, gk, gv)
    vR = (vu, vq, vk, vv)
    other = 1 - c

    loads = {}
    count = [0]

    def load(key, src, dst):
        copy = pltpu.make_async_copy(src, dst, load_sem.at[count[0]])
        count[0] += 1
        copy.start()
        loads.setdefault(key, []).append(copy)

    for src, dst in ((hnorm, gnorm), (hbias, gbias), (knorm, wnorm), (kbias, wbias)):
        load("v", src, dst)
    for h in range(2):
        for src, dst in zip(hR, fR):
            load(("R", h, 0), src.at[:, other, h], dst.at[:, other, h])
    for h in range(2):
        load(("C", h), gd.at[h], fd.at[h])
        load(("C", h), gm.at[h], fm.at[h])
    for h in range(2):
        for src, dst in zip(hR, fR):
            load(("R", h, 1), src.at[:, c, h], dst.at[:, c, h])
    for src, dst in ((wu, vu), (wq, vq), (wk, vk), (wv, vv)):
        load("wR", src, dst)
    for src, dst in ((wd, vd), (wm, vm)):
        load("wC", src, dst)

    def ready(key):
        for copy in loads[key]:
            copy.wait()

    barrier = pltpu.get_barrier_semaphore()
    for d in range(1, n):
        pl.semaphore_signal(barrier, inc=1, device_id={"batch": (b + d) % n}, device_id_type=MESH)
    for d in range(1, nz):
        pl.semaphore_signal(barrier, inc=1, device_id={"cols": (z + d) % nz}, device_id_type=MESH)
    pl.semaphore_wait(barrier, n - 1 + nz - 1)

    def remote(src, dst, send, recv, axis, target):
        return pltpu.make_async_remote_copy(
            src_ref=src, dst_ref=dst, send_sem=send, recv_sem=recv,
            device_id={axis: target}, device_id_type=MESH,
        )

    pending = []

    ready("v")
    for o in range(n):
        vsend[o, 0:1, :] = gnorm[0:1, o * LANES : (o + 1) * LANES]
        vsend[o, 1:2, :] = gbias[0:1, o * LANES : (o + 1) * LANES]
    vec_in = []
    for d in range(1, n):
        to = (b + d) % n
        copy = remote(vsend.at[to], vrecv.at[d], v_send.at[0, d], v_recv.at[0, d], "batch", to)
        copy.start()
        vec_in.append(copy)

    STEP = 16
    per = rows // STEP
    CSTEP = 128
    n_dn, n_mx = dn_r // CSTEP, mx_r // CSTEP

    def piece(h, q, core, part):
        return pl.ds(pl.multiple_of((2 * q + core) * LANES, LANES), LANES)

    chunks = [("R", 0), ("R", 1), ("C", 0), ("C", 1)]
    core_copies = []
    for i, (kind, h) in enumerate(chunks):
        if kind == "R":
            ready(("R", h, 0))

            def cast(t, _, h=h):
                q, r = t // per, pl.ds(pl.multiple_of((t % per) * STEP, STEP), STEP)
                for (lo, hi), f in zip(segs, fR):
                    s0R[h, q, r, lo:hi] = f[q, other, h, r, :].astype(jnp.bfloat16)
                return 0

            lax.fori_loop(0, n // 2 * per, cast, 0)
            copy = remote(s0R.at[h], r0R.at[h], rs_send.at[0, i], rs_recv.at[0, i], "batch", p_core)
        else:
            ready(("C", h))

            def cast(q, _, h=h):
                lanes = piece(h, q, other, 0)
                for k in range(n_dn):
                    r = slice(k * CSTEP, (k + 1) * CSTEP)
                    s0C[h, q, r, :] = fd[h, r, lanes].astype(jnp.bfloat16)
                for k in range(n_mx):
                    r = slice(k * CSTEP, (k + 1) * CSTEP)
                    s0C[h, q, dn_r + k * CSTEP : dn_r + (k + 1) * CSTEP, :] = fm[h, r, lanes].astype(jnp.bfloat16)
                return 0

            lax.fori_loop(0, n // 2, cast, 0)
            copy = remote(s0C.at[h], r0C.at[h], rs_send.at[0, i], rs_recv.at[0, i], "batch", p_core)
        copy.start()
        core_copies.append(copy)
        pending.append(copy)

    first = []
    for i, (kind, h) in enumerate(chunks):
        core_copies[i].wait_recv()
        if kind == "R":
            ready(("R", h, 1))

            def add(t, _, h=h):
                q, r = t // per, pl.ds(pl.multiple_of((t % per) * STEP, STEP), STEP)
                for (lo, hi), f in zip(segs, fR):
                    both = f[q, c, h, r, :] + r0R[h, q, r, lo:hi].astype(jnp.float32)
                    SR[h, q // 2, q % 2, r, lo:hi] = both.astype(jnp.bfloat16)
                return 0

            lax.fori_loop(0, n // 2 * per, add, 0)
            S, r1 = SR, r1R
        else:

            def add(q, _, h=h):
                lanes = piece(h, q, c, 0)
                for f, base, blocks in ((fd, 0, n_dn), (fm, dn_r, n_mx)):
                    for k in range(blocks):
                        here = slice(base + k * CSTEP, base + (k + 1) * CSTEP)
                        both = f[h, k * CSTEP : (k + 1) * CSTEP, lanes] + r0C[h, q, here, :].astype(jnp.float32)
                        SC[h, q // 2, q % 2, here, :] = both.astype(jnp.bfloat16)
                return 0

            lax.fori_loop(0, n // 2, add, 0)
            S, r1 = SC, r1C
        if h == 0:
            src, target = S.at[h, :, 1 - x], p_x
        else:
            src, target = S.at[h, 1 - y], p_y
        copy = remote(src, r1.at[h], rs_send.at[1, i], rs_recv.at[1, i], "batch", target)
        copy.start()
        first.append(copy)
        pending.append(copy)

    second = []
    for i, (kind, h) in enumerate(chunks):
        first[i].wait_recv()
        yy, xx, away, target = (1 - y, x, 1 - y, p_y) if h == 0 else (y, 1 - x, 1 - x, p_x)
        S, r1, t_, r2, blk, steps = (
            (SR, r1R, tR, r2R, STEP, per) if kind == "R" else (SC, r1C, tC, r2C, CSTEP, n_dn + n_mx)
        )

        def fold(k, _, h=h, yy=yy, xx=xx, away=away, S=S, r1=r1, t_=t_, blk=blk):
            r = pl.ds(pl.multiple_of(k * blk, blk), blk)
            both = S[h, yy, xx, r, :].astype(jnp.float32) + r1[h, away, r, :].astype(jnp.float32)
            t_[h, r, :] = both.astype(jnp.bfloat16)
            return 0

        lax.fori_loop(0, steps, fold, 0)
        copy = remote(t_.at[h], r2.at[h], rs_send.at[2, i], rs_recv.at[2, i], "batch", target)
        copy.start()
        second.append(copy)
        pending.append(copy)

    def mean_of(S, r1, r2, h, r):
        near = y if h == 0 else x
        total = S[h, y, x, r, :].astype(jnp.float32) + r1[h, near, r, :].astype(jnp.float32)
        return (total + r2[h, r, :].astype(jnp.float32)) * rate

    def spread(slot):
        copies = []
        for d in range(1, nz):
            copy = remote(
                st_send.at[slot], st_recv.at[slot, d], z_send.at[slot, d], z_recv.at[slot, d], "cols", (z + d) % nz
            )
            copy.start()
            copies.append(copy)
        return copies

    ready("wR")
    lane = lax.broadcasted_iota(jnp.int32, (STEP, LANES), 1)
    for h in range(2):
        second[h].wait_recv()

        def means(k, _, h=h):
            r = pl.ds(pl.multiple_of(k * STEP, STEP), STEP)
            mean = mean_of(SR, r1R, r2R, h, r)
            NR[h, r, :] = mean
            stats = jnp.zeros((STEP, LANES), jnp.float32)
            for j, ((lo, hi), v) in enumerate(zip(segs, vR)):
                w = v[h, r, :]
                own = jnp.sum(w * w, axis=1, keepdims=True)
                m = mean[:, lo:hi]
                slope = jnp.sum(m * m, axis=1, keepdims=True)
                stats = jnp.where(lane == j, own, stats)
                stats = jnp.where(lane == 4 + j, slope, stats)
            stm[pl.ds(pl.multiple_of(h * rows + k * STEP, STEP), STEP), :] = stats
            return 0

        lax.fori_loop(0, per, means, 0)
    st_send[0] = jnp.transpose(stm[...])[0:8, :]
    z_row = spread(0)

    total = vsend[b]
    for copy in vec_in:
        copy.wait_recv()
    for d in range(1, n):
        total = total + vrecv[d]
    old = jnp.concatenate([wnorm[...], wbias[...]], axis=0)
    NV[b] = old - learn_rate * (total * rate)
    vec_out = []
    for d in range(1, n):
        copy = remote(NV.at[b], NV.at[b], v_send.at[1, d], v_recv.at[1, d], "batch", (b + d) % n)
        copy.start()
        vec_out.append(copy)

    ready("wC")
    zero = jnp.zeros((1, LANES), jnp.float32)
    sums = [zero] * 4
    for h in range(2):
        second[2 + h].wait_recv()

        def means(k, carry, h=h, v=None, base=0):
            r = pl.ds(pl.multiple_of(base + k * CSTEP, CSTEP), CSTEP)
            mean = mean_of(SC, r1C, r2C, h, r)
            NC[h, r, :] = mean
            w = v[h, pl.ds(pl.multiple_of(k * CSTEP, CSTEP), CSTEP), :]
            own, slope = carry
            return (
                own + jnp.sum(w * w, axis=0, keepdims=True),
                slope + jnp.sum(mean * mean, axis=0, keepdims=True),
            )

        sums[0], sums[2] = lax.fori_loop(
            0, n_dn, functools.partial(means, v=vd, base=0), (sums[0], sums[2])
        )
        sums[1], sums[3] = lax.fori_loop(
            0, n_mx, functools.partial(means, v=vm, base=dn_r), (sums[1], sums[3])
        )
    st_send[1] = jnp.concatenate(sums + [zero] * 4, axis=0)
    z_col = spread(1)

    def ratio_of(slot, copies, number):
        for copy in copies:
            copy.wait_recv()
        total = st_send[slot]
        for d in range(1, nz):
            total = total + st_recv[slot, d]
        return jnp.sqrt(total[0:number]) * lax.rsqrt(total[number : 2 * number] + 1e-06)

    ag = {}

    def share(i, G, slot, step, axis_target):
        copy = remote(
            G.at[slot, chunks[i][1]], G.at[slot, chunks[i][1]],
            ag_send.at[i, step], ag_recv.at[i, step], "batch", axis_target,
        )
        copy.start()
        ag[i, step] = copy

    def own_out(i, G):
        h = chunks[i][1]
        near, far = (p_y, p_x) if h == 0 else (p_x, p_y)
        share(i, G, b, 0, near)
        share(i, G, b, 1, far)
        share(i, G, b, 3, p_core)

    ratio = ratio_of(0, z_row, 4)
    stm[...] = jnp.transpose(jnp.concatenate([ratio, jnp.zeros((LANES - 4, LANES), jnp.float32)], axis=0))
    for h in range(2):

        def update(k, _, h=h):
            r = pl.ds(pl.multiple_of(k * STEP, STEP), STEP)
            scale = stm[pl.ds(pl.multiple_of(h * rows + k * STEP, STEP), STEP), :]
            for j, ((lo, hi), v) in enumerate(zip(segs, vR)):
                new = v[h, r, :] - learn_rate * (NR[h, r, lo:hi] * scale[:, j : j + 1])
                NR[h, r, lo:hi] = new
                GR[b, h, r, lo:hi] = new.astype(jnp.bfloat16)
            return 0

        lax.fori_loop(0, per, update, 0)
        own_out(h, GR)

    ratio = ratio_of(1, z_col, 2)
    for h in range(2):
        for j, (v, base, blocks) in enumerate(((vd, 0, n_dn), (vm, dn_r, n_mx))):

            def update(k, _, h=h, j=j, v=v, base=base):
                r = pl.ds(pl.multiple_of(base + k * CSTEP, CSTEP), CSTEP)
                w = v[h, pl.ds(pl.multiple_of(k * CSTEP, CSTEP), CSTEP), :]
                new = w - learn_rate * (NC[h, r, :] * ratio[j : j + 1, :])
                NC[h, r, :] = new
                GC[b, h, r, :] = new.astype(jnp.bfloat16)
                return 0

            lax.fori_loop(0, blocks, update, 0)
        own_out(2 + h, GC)

    for pair in ((0, 1), (2, 3)):
        for i in pair:
            h, G = chunks[i][1], GR if i < 2 else GC
            near, far = (p_y, p_x) if h == 0 else (p_x, p_y)
            ag[i, 0].wait_recv()
            share(i, G, near, 2, far)
            share(i, G, near, 4, p_core)
        for i in pair:
            h, G = chunks[i][1], GR if i < 2 else GC
            far = p_x if h == 0 else p_y
            ag[i, 1].wait_recv()
            share(i, G, far, 5, p_core)
    across = p_x + p_y - b
    for i in range(4):
        ag[i, 2].wait_recv()
        share(i, GR if i < 2 else GC, across, 6, p_core)
    for i in range(4):
        for step in range(3, 7):
            ag[i, step].wait_recv()
        for step in range(7):
            ag[i, step].wait_send()
    for copy in vec_out:
        copy.wait_recv()
        copy.wait_send()
    for copy in vec_in + z_row + z_col + pending:
        copy.wait_send()


def write_kernel(dims, GR, GC, NR, NC, NV, cu, cd, cq, ck, cv, cm, cn, cb, nu, nd, nq, nk, nv, nm, nn, nb, sem):
    rows, up_w, at_w, dn_r, mx_r = dims
    n = GR.shape[0]
    b = lax.axis_index("batch")
    copies = []

    def go(src, dst):
        copy = pltpu.make_async_copy(src, dst, sem.at[len(copies)])
        copy.start()
        copies.append(copy)

    for o in range(n):
        lanes = pl.ds(o * LANES, LANES)
        go(GC.at[o, :, 0:dn_r, :], cd.at[:, :, lanes])
        go(GC.at[o, :, dn_r : dn_r + mx_r, :], cm.at[:, :, lanes])
    go(GR.at[:, :, :, 0:up_w], cu)
    go(NR.at[:, :, 0:up_w], nu)
    for j, (copied, new) in enumerate(((cq, nq), (ck, nk), (cv, nv))):
        lanes = slice(up_w + j * at_w, up_w + (j + 1) * at_w)
        go(GR.at[:, :, :, lanes], copied)
        go(NR.at[:, :, lanes], new)
    go(NC.at[:, 0:dn_r], nd)
    go(NC.at[:, dn_r : dn_r + mx_r], nm)
    for o in range(n):
        both = NV[o]
        cn[0:1, o * LANES : (o + 1) * LANES] = both[0:1].astype(jnp.bfloat16)
        cb[0:1, o * LANES : (o + 1) * LANES] = both[1:2].astype(jnp.bfloat16)
    own = NV[b]
    nn[...] = own[0:1]
    nb[...] = own[1:2]
    for copy in copies:
        copy.wait()


def fused(
    grad_up, grad_down, grad_query, grad_key, grad_value, grad_mixed, grad_norm, grad_bias,
    weight_up, weight_down, weight_query, weight_key, weight_value, weight_mixed, weight_norm, weight_bias,
):
    n, nz = lax.axis_size("batch"), lax.axis_size("cols")
    f32, bf16 = jnp.float32, jnp.bfloat16
    rows = weight_up.shape[0] // 2
    up_w, at_w = weight_up.shape[1], weight_query.shape[1]
    dn_r, mx_r = weight_down.shape[0] // 2, weight_mixed.shape[0] // 2
    dims = (rows, up_w, at_w, dn_r, mx_r)
    row_w, col_r = up_w + 3 * at_w, dn_r + mx_r
    chips = n // 2

    def by_row(g):
        return g[0].reshape(chips, 2, 2, rows, g.shape[2])

    def halves(a):
        return a.reshape(2, a.shape[0] // 2, a.shape[1])

    HB = pl.BlockSpec(memory_space=pltpu.MemorySpace.HBM)
    VM = pl.BlockSpec(memory_space=pltpu.VMEM)
    DMA = pltpu.SemaphoreType.DMA
    mid = [
        pltpu.VMEM((n, 2, rows, row_w), bf16),
        pltpu.VMEM((n, 2, col_r, LANES), bf16),
        pltpu.VMEM((2, rows, row_w), f32),
        pltpu.VMEM((2, col_r, LANES), f32),
        pltpu.VMEM((n, 2, LANES), f32),
    ]
    scratch = [pltpu.VMEM((chips, 2, 2, rows, w), f32) for w in (up_w, at_w, at_w, at_w)]
    scratch += [pltpu.VMEM((2, r, n * LANES), f32) for r in (dn_r, mx_r)]
    scratch += [pltpu.VMEM((2, rows, w), f32) for w in (up_w, at_w, at_w, at_w)]
    scratch += [pltpu.VMEM((2, r, LANES), f32) for r in (dn_r, mx_r)]
    R, C = (rows, row_w), (col_r, LANES)
    for lead in ((2, chips), (2, chips), (2, 2, 2), (2, 2), (2,), (2,)):
        scratch += [pltpu.VMEM(lead + R, bf16), pltpu.VMEM(lead + C, bf16)]
    scratch += [
        pltpu.VMEM((n, 2, LANES), f32),
        pltpu.VMEM((n, 2, LANES), f32),
        pltpu.VMEM((2 * rows, LANES), f32),
        pltpu.VMEM((2, 8, LANES), f32),
        pltpu.VMEM((2, nz, 8, LANES), f32),
        pltpu.VMEM((1, n * LANES), f32), pltpu.VMEM((1, n * LANES), f32),
        pltpu.VMEM((1, LANES), f32), pltpu.VMEM((1, LANES), f32),
        DMA((30,)), DMA((3, 4)), DMA((3, 4)), DMA((2, nz)), DMA((2, nz)),
        DMA((2, n)), DMA((2, n)), DMA((4, 7)), DMA((4, 7)),
    ]
    got = pl.pallas_call(
        functools.partial(gather_kernel, n, nz, dims),
        out_shape=mid,
        in_specs=[HB] * 16,
        out_specs=[VM] * 5,
        scratch_shapes=scratch,
        compiler_params=pltpu.CompilerParams(
            collective_id=0, has_side_effects=True, vmem_limit_bytes=VMEM_BYTES
        ),
        name="sum_and_share",
    )(*(pltpu.with_memory_space_constraint(a, pltpu.MemorySpace.HBM) for a in (
        by_row(grad_up), by_row(grad_query), by_row(grad_key), by_row(grad_value),
        halves(grad_down[0]), halves(grad_mixed[0]), grad_norm, grad_bias,
        halves(weight_up), halves(weight_query), halves(weight_key), halves(weight_value),
        halves(weight_down), halves(weight_mixed), weight_norm[None], weight_bias[None],
    )))
    S = jax.ShapeDtypeStruct
    width = n * LANES
    outs = pl.pallas_call(
        functools.partial(write_kernel, dims),
        out_shape=[
            S((n, 2, rows, up_w), bf16), S((2, dn_r, width), bf16),
            S((n, 2, rows, at_w), bf16), S((n, 2, rows, at_w), bf16), S((n, 2, rows, at_w), bf16),
            S((2, mx_r, width), bf16), S((1, width), bf16), S((1, width), bf16),
            S((2, rows, up_w), f32), S((2, dn_r, LANES), f32),
            S((2, rows, at_w), f32), S((2, rows, at_w), f32), S((2, rows, at_w), f32),
            S((2, mx_r, LANES), f32), S((1, LANES), f32), S((1, LANES), f32),
        ],
        in_specs=[VM] * 5,
        out_specs=[HB] * 6 + [VM] * 2 + [HB] * 6 + [VM] * 2,
        scratch_shapes=[DMA((26,))],
        compiler_params=pltpu.CompilerParams(vmem_limit_bytes=VMEM_BYTES // 10),
        name="write_out",
    )(*(pltpu.with_memory_space_constraint(a, pltpu.MemorySpace.VMEM) for a in got))
    shapes = [
        (n * 2 * rows, up_w), (2 * dn_r, width), (n * 2 * rows, at_w), (n * 2 * rows, at_w),
        (n * 2 * rows, at_w), (2 * mx_r, width), (width,), (width,),
        weight_up.shape, weight_down.shape, weight_query.shape, weight_key.shape,
        weight_value.shape, weight_mixed.shape, weight_norm.shape, weight_bias.shape,
    ]
    return tuple(out.reshape(shape) for out, shape in zip(outs, shapes))


def solution(mesh):
    in_specs = (
        P("batch", None, "cols"),
        P("batch", "cols", None),
        P("batch", None, "cols"),
        P("batch", None, "cols"),
        P("batch", None, "cols"),
        P("batch", "cols", None),
        P("batch", None),
        P("batch", None),
        P("batch", "cols"),
        P("cols", "batch"),
        P("batch", "cols"),
        P("batch", "cols"),
        P("batch", "cols"),
        P("cols", "batch"),
        P("batch"),
        P("batch"),
    )
    out_specs = (
        P(None, "cols"),
        P("cols", None),
        P(None, "cols"),
        P(None, "cols"),
        P(None, "cols"),
        P("cols", None),
        P(),
        P(),
        P("batch", "cols"),
        P("cols", "batch"),
        P("batch", "cols"),
        P("batch", "cols"),
        P("batch", "cols"),
        P("cols", "batch"),
        P("batch"),
        P("batch"),
    )
    whole = mesh.shape["batch"]

    def chosen(*arrays):
        width = arrays[15].shape[0]
        fits = whole == 8 and width == LANES and all(
            side % LANES == 0 for array in arrays[:6] for side in array.shape[1:]
        )
        return (fused if fits else local)(*arrays)

    return jax.shard_map(chosen, mesh=mesh, in_specs=in_specs, out_specs=out_specs, check_vma=False)
```
